32 devices in a mesh: dp: 4 (over x, y), ep: 8 (over z, core).
Axes of the slice: x: 2, y: 2, z: 4, core: 2. Of those that a mesh axis runs over, the one named last changes fastest.
Arguments:
- hidden: bfloat16 [65536, 2048], P(('dp', 'ep')), parts along dimension 0
- ln_gamma: float32 [2048], replicated
- ln_beta: float32 [2048], replicated
- w_router: bfloat16 [2048, 8], replicated
- w_gate: bfloat16 [8, 2048, 5632], P('ep')
- w_up: bfloat16 [8, 2048, 5632], P('ep')
- w_down: bfloat16 [8, 5632, 2048], P('ep')
- choice: int32 [65536, 2], P(('dp', 'ep')), parts along dimension 0
- mask_first: int32 [65536, 8], P(('dp', 'ep')), parts along dimension 0
- mask_second: int32 [65536, 8], P(('dp', 'ep')), parts along dimension 0
Outputs:
- output: bfloat16 [65536, 2048], P(('dp', 'ep')), parts along dimension 0
There are 4 independent parts. The reference program is written for one: setup_inputs(seed, part) draws one part's arguments, and reference() takes and returns one part's arrays. A program takes and returns all parts, laid end to end along the dimension named above; an argument that names none is the same for every part.
All inputs are finite; a program needn't handle non-finite values.
Results may differ from the reference program's by a relative error of at most 0.00104.
Values are sent between devices in bfloat16 or wider.
A program may use at most 1 GiB of HBM per device.

```python
import jax
import jax.numpy as jnp
from jax import lax

D_MODEL = 2048
FF_WIDTH = 5632
EXPERTS = 8
TOKENS_DEV = 2048
GROUP_DEVS = 8
TOKENS = GROUP_DEVS * TOKENS_DEV
CAPACITY = (10 * TOKENS_DEV + 4 * EXPERTS - 1) // (4 * EXPERTS)
LN_EPS = 1e-5


def draw_routing(route_key):
    sub_keys = jax.random.split(route_key, 6)
    favoured = jax.random.randint(sub_keys[0], (), 0, EXPERTS)
    coin_flip = jax.random.randint(sub_keys[1], (TOKENS,), 0, 4)
    spread = jax.random.randint(sub_keys[2], (TOKENS,), 0, EXPERTS)
    first_pick = jnp.where(coin_flip == 0, favoured, spread)
    second_pick = (first_pick + 1 + jax.random.randint(sub_keys[3], (TOKENS,), 0, EXPERTS - 1)) % EXPERTS
    expert_ids = jnp.arange(EXPERTS)
    is_first = first_pick[:, None] == expert_ids
    is_second = second_pick[:, None] == expert_ids
    keep_first = jax.random.randint(sub_keys[4], (TOKENS, EXPERTS), 0, 4) == 0
    keep_second = jax.random.randint(sub_keys[5], (TOKENS, EXPERTS), 0, 4) == 0
    mask_first = (keep_first | is_first).astype(jnp.int32)
    mask_second = ((keep_second | is_second) & (~is_first)).astype(jnp.int32)
    choice = jnp.stack([first_pick, second_pick], axis=1).astype(jnp.int32)
    return choice, mask_first, mask_second


def setup_inputs(seed: int = 0, part: int = 0) -> dict:
    shared_keys = jax.random.split(jax.random.key(seed), 6)
    part_keys = jax.random.split(jax.random.fold_in(jax.random.key(seed + 1), part), 2)
    hidden = jax.random.normal(part_keys[0], (TOKENS, D_MODEL), jnp.float32).astype(jnp.bfloat16)
    choice, mask_first, mask_second = draw_routing(part_keys[1])
    ln_gamma = 1.0 + 0.4 * jax.random.normal(shared_keys[0], (D_MODEL,), jnp.float32)
    ln_beta = 0.4 * jax.random.normal(shared_keys[1], (D_MODEL,), jnp.float32)
    w_router = (jax.random.normal(shared_keys[2], (D_MODEL, EXPERTS), jnp.float32) * D_MODEL ** -0.5).astype(jnp.bfloat16)
    w_gate = (jax.random.normal(shared_keys[3], (EXPERTS, D_MODEL, FF_WIDTH), jnp.float32) * D_MODEL ** -0.5).astype(jnp.bfloat16)
    w_up = (jax.random.normal(shared_keys[4], (EXPERTS, D_MODEL, FF_WIDTH), jnp.float32) * D_MODEL ** -0.5).astype(jnp.bfloat16)
    w_down = (jax.random.normal(shared_keys[5], (EXPERTS, FF_WIDTH, D_MODEL), jnp.float32) * FF_WIDTH ** -0.5).astype(jnp.bfloat16)
    return {"hidden": hidden, "ln_gamma": ln_gamma, "ln_beta": ln_beta, "w_router": w_router,
            "w_gate": w_gate, "w_up": w_up, "w_down": w_down, "choice": choice,
            "mask_first": mask_first, "mask_second": mask_second}


def layer_norm(token_rows, ln_gamma, ln_beta):
    values = token_rows.astype(jnp.float32)
    centred = values - jnp.mean(values, axis=-1, keepdims=True)
    variance = jnp.mean(centred * centred, axis=-1, keepdims=True)
    return (centred * lax.rsqrt(variance + LN_EPS) * ln_gamma + ln_beta).astype(jnp.bfloat16)


def reference(hidden, ln_gamma, ln_beta, w_router, w_gate, w_up, w_down, choice, mask_first, mask_second):
    normed = layer_norm(hidden, ln_gamma, ln_beta)
    scores = jnp.dot(normed, w_router, preferred_element_type=jnp.float32)
    mask_pair = jnp.stack([mask_first, mask_second], axis=1) > 0
    soft_probs = jax.nn.softmax(jnp.where(mask_pair, scores[:, None, :], -jnp.inf), axis=-1)
    gate_vals = jnp.take_along_axis(soft_probs, choice[:, :, None], axis=-1)[:, :, 0]
    by_source = choice.reshape(GROUP_DEVS, TOKENS_DEV, 2)
    expert_ids = jnp.arange(EXPERTS, dtype=jnp.int32)
    hit_count = (by_source[..., None] == expert_ids).astype(jnp.int32)
    per_token = jnp.sum(hit_count, axis=2)
    before = jnp.cumsum(per_token, axis=1) - per_token
    position = jnp.take_along_axis(before, by_source, axis=2)
    kept_copy = position < CAPACITY
    source_ids = jnp.broadcast_to(jnp.arange(GROUP_DEVS, dtype=jnp.int32)[:, None, None], by_source.shape)
    token_ids = jnp.broadcast_to(jnp.arange(TOKENS, dtype=jnp.int32).reshape(GROUP_DEVS, TOKENS_DEV, 1), by_source.shape)
    slot_table = jnp.zeros((EXPERTS, GROUP_DEVS, CAPACITY), jnp.int32)
    slot_table = slot_table.at[by_source, source_ids, position].set(token_ids, mode="drop")

    def one_expert(operands):
        row_index, gate_mat, up_mat, down_mat = operands
        expert_rows = normed[row_index.reshape(-1)]
        gate_proj = jnp.dot(expert_rows, gate_mat, preferred_element_type=jnp.float32)
        up_proj = jnp.dot(expert_rows, up_mat, preferred_element_type=jnp.float32)
        inner_act = (jax.nn.silu(gate_proj) * up_proj).astype(jnp.bfloat16)
        return jnp.dot(inner_act, down_mat, preferred_element_type=jnp.float32).astype(jnp.bfloat16)

    expert_out = lax.map(one_expert, (slot_table, w_gate, w_up, w_down))
    expert_out = expert_out.reshape(EXPERTS, GROUP_DEVS, CAPACITY, D_MODEL)
    picked = expert_out[by_source, source_ids, jnp.minimum(position, CAPACITY - 1)]
    kept_gates = jnp.where(kept_copy, gate_vals.reshape(GROUP_DEVS, TOKENS_DEV, 2), 0.0)
    mixed_out = hidden.reshape(GROUP_DEVS, TOKENS_DEV, D_MODEL).astype(jnp.float32) + jnp.sum(kept_gates[..., None] * picked.astype(jnp.float32), axis=2)
    return mixed_out.reshape(TOKENS, D_MODEL).astype(jnp.bfloat16)
```

```python
import functools

import jax
import jax.numpy as jnp
from jax import lax
from jax.experimental import pallas as pl
from jax.experimental.pallas import tpu as pltpu
from jax.sharding import PartitionSpec as P

LN_EPS = 1e-5
MESH = pl.DeviceIdType.MESH


def layer_norm(token_rows, ln_gamma, ln_beta):
    values = token_rows.astype(jnp.float32)
    centred = values - jnp.mean(values, axis=-1, keepdims=True)
    variance = jnp.mean(centred * centred, axis=-1, keepdims=True)
    return (centred * lax.rsqrt(variance + LN_EPS) * ln_gamma + ln_beta).astype(jnp.bfloat16)


def sparse_gates(normed, w_router, choice, mask_first, mask_second):
    scores = jnp.dot(normed, w_router, preferred_element_type=jnp.float32)
    expert_ids = jnp.arange(w_router.shape[1], dtype=jnp.int32)
    mask_pair = jnp.stack([mask_first, mask_second], axis=1) > 0
    soft_probs = jax.nn.softmax(jnp.where(mask_pair, scores[:, None, :], -jnp.inf), axis=-1)
    return jnp.sum(jnp.where(choice[:, :, None] == expert_ids, soft_probs, 0.0), axis=-1)


def xor(a, b, n):
    total, bit = 0, 1
    while bit < n:
        p, q = (a // bit) % 2, (b // bit) % 2
        total = total + bit * (p + q - 2 * p * q)
        bit *= 2
    return total


def visit(i):
    return i + (i // 4) * (2 - 4 * ((i // 2) % 2))


def moe_kernel(n, cap, ft, tc, pos_row, pos_col, gate_col, u_hbm, x_hbm, wg, wu, wd,
               out, sbuf, rbuf, ybuf, bbuf,
               ubuf, pmat, temp, xin, acc, wgb, wub, wdb, oacc,
               send_sem, recv_sem, ysend_sem, yrecv_sem, wsem, lsem, osem):
    me = lax.axis_index("ep")
    tokens, width = ubuf.shape
    nf = wg.shape[1] // ft
    ncol = width // 512
    bf16, f32 = jnp.bfloat16, jnp.float32

    u_copy = pltpu.make_async_copy(u_hbm, ubuf, lsem.at[0])
    u_copy.start()

    def weight_copies(f, slot):
        cols = pl.ds(pl.multiple_of(f * ft, ft), ft)
        return (pltpu.make_async_copy(wg.at[:, cols], wgb.at[slot], wsem.at[slot, 0]),
                pltpu.make_async_copy(wu.at[:, cols], wub.at[slot], wsem.at[slot, 1]),
                pltpu.make_async_copy(wd.at[cols, :], wdb.at[slot], wsem.at[slot, 2]))

    for c in weight_copies(0, 0):
        c.start()

    barrier = pltpu.get_barrier_semaphore()

    def greet(k, _):
        pl.semaphore_signal(barrier, inc=1, device_id={"ep": xor(me, k, n)}, device_id_type=MESH)
        return 0

    lax.fori_loop(1, n, greet, 0)
    pl.semaphore_wait(barrier, n - 1)
    u_copy.wait()

    def send_copy(k):
        return pltpu.make_async_remote_copy(
            src_ref=sbuf.at[k], dst_ref=rbuf.at[k], send_sem=send_sem.at[k], recv_sem=recv_sem.at[k],
            device_id={"ep": xor(me, k, n)}, device_id_type=MESH)

    def back_copy(k):
        return pltpu.make_async_remote_copy(
            src_ref=ybuf.at[k], dst_ref=bbuf.at[k], send_sem=ysend_sem.at[k], recv_sem=yrecv_sem.at[k],
            device_id={"ep": xor(me, k, n)}, device_id_type=MESH)

    inner = ((me // 2 + 1) // 2) % 2

    def dispatch(i, _):
        pair, odd = i // 2, i % 2
        first = 1 + 2 * inner
        second = 3 - 2 * inner
        code = ((pair == 0).astype(jnp.int32) * first + (pair == 1).astype(jnp.int32) * second
                + (pair == 2).astype(jnp.int32) * 2)
        k = jnp.where(pair == 3, 1 - odd, 2 * code + odd)
        slot_ids = lax.broadcasted_iota(jnp.int32, (cap, tokens), 0)
        pmat[...] = jnp.where(slot_ids == pos_row[pl.ds(k, 1), :], 1.0, 0.0).astype(bf16)

        def column(c, _):
            cols = pl.ds(pl.multiple_of(c * 512, 512), 512)
            temp[:, cols] = jnp.dot(pmat[...], ubuf[:, cols], preferred_element_type=f32).astype(bf16)
            return 0

        lax.fori_loop(0, ncol, column, 0)

        @pl.when(k == 0)
        def _():
            own = pltpu.make_async_copy(temp, rbuf.at[0], lsem.at[1])
            own.start()
            own.wait()

        @pl.when(k > 0)
        def _():
            stage = pltpu.make_async_copy(temp, sbuf.at[k], lsem.at[1])
            stage.start()
            stage.wait()
            send_copy(k).start()

        return 0

    lax.fori_loop(0, n, dispatch, 0)

    x_copy = pltpu.make_async_copy(x_hbm, ubuf, lsem.at[0])
    x_copy.start()

    def mlp(t, _):
        i, f, slot = t // nf, t % nf, t % 2
        k = visit(i)

        @pl.when(f == 0)
        def _():
            @pl.when(k > 0)
            def _():
                send_copy(k).wait_recv()

            load = pltpu.make_async_copy(rbuf.at[k], xin, lsem.at[1])
            load.start()
            load.wait()
            acc[...] = jnp.zeros_like(acc)

        for c in weight_copies(f, slot):
            c.wait()

        @pl.when(t + 1 < n * nf)
        def _():
            for c in weight_copies((t + 1) % nf, (t + 1) % 2):
                c.start()

        gate_proj = jnp.dot(xin[...], wgb[slot], preferred_element_type=f32)
        up_proj = jnp.dot(xin[...], wub[slot], preferred_element_type=f32)
        inner_act = (jax.nn.silu(gate_proj) * up_proj).astype(bf16)
        for c in range(ncol):
            cols = slice(c * 512, (c + 1) * 512)
            acc[:, cols] += jnp.dot(inner_act, wdb[slot, :, cols], preferred_element_type=f32)

        @pl.when(f == nf - 1)
        def _():
            temp[...] = acc[...].astype(bf16)

            @pl.when(k == 0)
            def _():
                own = pltpu.make_async_copy(temp, bbuf.at[0], lsem.at[1])
                own.start()
                own.wait()

            @pl.when(k > 0)
            def _():
                stage = pltpu.make_async_copy(temp, ybuf.at[k], lsem.at[1])
                stage.start()
                stage.wait()
                back_copy(k).start()

        return 0

    lax.fori_loop(0, n * nf, mlp, 0)
    x_copy.wait()

    def out_copy(r):
        rows = pl.ds(pl.multiple_of(r * tc, tc), tc)
        return pltpu.make_async_copy(ubuf.at[rows, :], out.at[rows, :], osem.at[r])

    def combine(i, _):
        k = visit(i)

        @pl.when(k > 0)
        def _():
            back_copy(k).wait_recv()

        load = pltpu.make_async_copy(bbuf.at[k], xin, lsem.at[1])
        load.start()
        load.wait()

        def rows_step(r, _):
            rows = pl.ds(pl.multiple_of(r * tc, tc), tc)
            lane = lax.broadcasted_iota(jnp.int32, (tc, n), 1)
            pos = jnp.sum(jnp.where(lane == k, pos_col[rows, :], 0), axis=1, keepdims=True)
            gate = jnp.sum(jnp.where(lane == k, gate_col[rows, :], 0.0), axis=1, keepdims=True)
            slot_ids = lax.broadcasted_iota(jnp.int32, (tc, cap), 1)
            pick = jnp.where(slot_ids == pos, 1.0, 0.0).astype(bf16)

            @pl.when(i == 0)
            def _():
                oacc[rows, :] = ubuf[rows, :].astype(f32)

            for c in range(ncol):
                cols = slice(c * 512, (c + 1) * 512)
                picked = jnp.dot(pick, xin[:, cols], preferred_element_type=f32)
                oacc[rows, cols] += gate * picked

            @pl.when(i == n - 1)
            def _():
                ubuf[rows, :] = oacc[rows, :].astype(bf16)
                out_copy(r).start()

            return 0

        lax.fori_loop(0, tokens // tc, rows_step, 0)
        return 0

    lax.fori_loop(0, n, combine, 0)

    def finish(k, _):
        send_copy(k).wait_send()
        back_copy(k).wait_send()
        return 0

    lax.fori_loop(1, n, finish, 0)

    def drain(r, _):
        out_copy(r).wait()
        return 0

    lax.fori_loop(0, tokens // tc, drain, 0)


def solution(mesh):
    group_size = mesh.shape["ep"]
    rows_spec = P(("dp", "ep"))

    def device_step(hidden, ln_gamma, ln_beta, w_router, w_gate, w_up, w_down, choice, mask_first, mask_second):
        tokens, width = hidden.shape
        n = group_size
        ff = w_gate.shape[2]
        cap = (10 * tokens + 4 * n - 1) // (4 * n)
        ft, tc = 512, 256
        normed = layer_norm(hidden, ln_gamma, ln_beta)
        gate_vals = sparse_gates(normed, w_router, choice, mask_first, mask_second)
        experts = lax.axis_index("ep").astype(jnp.int32) ^ jnp.arange(n, dtype=jnp.int32)
        hit = choice[..., None] == experts
        hit_any = jnp.sum(hit.astype(jnp.int32), axis=1)
        before = jnp.cumsum(hit_any, axis=0) - hit_any
        kept = (hit_any > 0) & (before < cap)
        pos = jnp.where(kept, before, -1)
        gates = jnp.where(kept, jnp.sum(jnp.where(hit, gate_vals[..., None], 0.0), axis=1), 0.0)
        block = jax.ShapeDtypeStruct((n, cap, width), jnp.bfloat16)
        vmem = pl.BlockSpec(memory_space=pltpu.VMEM)
        hbm = pl.BlockSpec(memory_space=pl.ANY)
        bf16, f32 = jnp.bfloat16, jnp.float32
        return pl.pallas_call(
            functools.partial(moe_kernel, n, cap, ft, tc),
            out_shape=(jax.ShapeDtypeStruct((tokens, width), bf16), block, block, block, block),
            in_specs=[vmem] * 3 + [hbm] * 5,
            out_specs=(hbm,) * 5,
            scratch_shapes=[
                pltpu.VMEM((tokens, width), bf16),
                pltpu.VMEM((cap, tokens), bf16),
                pltpu.VMEM((cap, width), bf16),
                pltpu.VMEM((cap, width), bf16),
                pltpu.VMEM((cap, width), f32),
                pltpu.VMEM((2, width, ft), bf16),
                pltpu.VMEM((2, width, ft), bf16),
                pltpu.VMEM((2, ft, width), bf16),
                pltpu.VMEM((tokens, width), f32),
                pltpu.SemaphoreType.DMA((n,)),
                pltpu.SemaphoreType.DMA((n,)),
                pltpu.SemaphoreType.DMA((n,)),
                pltpu.SemaphoreType.DMA((n,)),
                pltpu.SemaphoreType.DMA((2, 3)),
                pltpu.SemaphoreType.DMA((2,)),
                pltpu.SemaphoreType.DMA((tokens // tc,)),
            ],
            compiler_params=pltpu.CompilerParams(
                collective_id=0, has_side_effects=True, vmem_limit_bytes=67043328),
            cost_estimate=pl.CostEstimate(
                flops=6 * n * cap * width * ff, bytes_accessed=n * 6 * width * ff, transcendentals=0),
        )(pos.T, pos, gates, normed, hidden, w_gate[0], w_up[0], w_down[0])[0]

    return jax.shard_map(device_step, mesh=mesh,
                         in_specs=(rows_spec, P(), P(), P(), P("ep"), P("ep"), P("ep"), rows_spec, rows_spec, rows_spec),
                         out_specs=rows_spec, check_vma=False)
```

```python
import functools

import jax
import jax.numpy as jnp
from jax import lax
from jax.experimental import pallas as pl
from jax.experimental.pallas import tpu as pltpu
from jax.sharding import PartitionSpec as P

LN_EPS = 1e-5
MESH = pl.DeviceIdType.MESH


def layer_norm(token_rows, ln_gamma, ln_beta):
    values = token_rows.astype(jnp.float32)
    centred = values - jnp.mean(values, axis=-1, keepdims=True)
    variance = jnp.mean(centred * centred, axis=-1, keepdims=True)
    return (centred * lax.rsqrt(variance + LN_EPS) * ln_gamma + ln_beta).astype(jnp.bfloat16)


def sparse_gates(normed, w_router, choice, mask_first, mask_second):
    scores = jnp.dot(normed, w_router, preferred_element_type=jnp.float32)
    expert_ids = jnp.arange(w_router.shape[1], dtype=jnp.int32)
    mask_pair = jnp.stack([mask_first, mask_second], axis=1) > 0
    soft_probs = jax.nn.softmax(jnp.where(mask_pair, scores[:, None, :], -jnp.inf), axis=-1)
    return jnp.sum(jnp.where(choice[:, :, None] == expert_ids, soft_probs, 0.0), axis=-1)


def xor(a, b, n):
    total, bit = 0, 1
    while bit < n:
        p, q = (a // bit) % 2, (b // bit) % 2
        total = total + bit * (p + q - 2 * p * q)
        bit *= 2
    return total


def moe_kernel(n, cap, ft, tc, pos_row, pos_col, gate_col, u_hbm, x_hbm, wg, wu, wd,
               out, sbuf, rbuf, ybuf, bbuf, ufar, fbuf,
               ubuf, pmat, temp, xin, acc, wgb, wub, wdb, oacc, posfar,
               send_sem, recv_sem, ysend_sem, yrecv_sem, usend_sem, urecv_sem, fsend_sem, wsem, lsem, osem, go_sem):
    me = lax.axis_index("ep")
    tokens, width = ubuf.shape
    nf = wg.shape[1] // ft
    ncol = width // 512
    bf16, f32 = jnp.bfloat16, jnp.float32
    inner = ((me // 2 + 1) // 2) % 2

    def visit(i):
        return i + inner * (i // 4) * (2 - 4 * ((i // 2) % 2))

    def gather_back(i):
        return i + (1 - inner) * (i // 4) * (2 - 4 * ((i // 2) % 2))

    u_copy = pltpu.make_async_copy(u_hbm, ubuf, lsem.at[0])
    u_copy.start()

    def weight_copies(f, slot):
        cols = pl.ds(pl.multiple_of(f * ft, ft), ft)
        return (pltpu.make_async_copy(wg.at[:, cols], wgb.at[slot], wsem.at[slot, 0]),
                pltpu.make_async_copy(wu.at[:, cols], wub.at[slot], wsem.at[slot, 1]),
                pltpu.make_async_copy(wd.at[cols, :], wdb.at[slot], wsem.at[slot, 2]))

    for c in weight_copies(0, 0):
        c.start()

    barrier = pltpu.get_barrier_semaphore()

    def greet(k, _):
        pl.semaphore_signal(barrier, inc=1, device_id={"ep": xor(me, k, n)}, device_id_type=MESH)
        return 0

    lax.fori_loop(1, n, greet, 0)
    pl.semaphore_wait(barrier, n - 1)

    def far_rows(slot):
        return pltpu.make_async_remote_copy(
            src_ref=u_hbm, dst_ref=ufar.at[slot], send_sem=usend_sem.at[0], recv_sem=urecv_sem.at[slot, 0],
            device_id={"ep": xor(me, 4 + 2 * inner, n)}, device_id_type=MESH)

    def far_slots(slot):
        return pltpu.make_async_remote_copy(
            src_ref=pos_row, dst_ref=posfar.at[slot], send_sem=usend_sem.at[1], recv_sem=urecv_sem.at[slot, 1],
            device_id={"ep": xor(me, 4 + 2 * inner, n)}, device_id_type=MESH)

    @pl.when(inner == 1)
    def _():
        far_rows(0).start()

    far_slots(1 - inner).start()
    u_copy.wait()

    def send_copy(k):
        return pltpu.make_async_remote_copy(
            src_ref=sbuf.at[k], dst_ref=rbuf.at[k], send_sem=send_sem.at[k], recv_sem=recv_sem.at[k],
            device_id={"ep": xor(me, k, n)}, device_id_type=MESH)

    def forward_copy(slot, j):
        k = xor(6 - 2 * slot, j, n)
        return pltpu.make_async_remote_copy(
            src_ref=fbuf.at[slot, j], dst_ref=rbuf.at[k], send_sem=fsend_sem.at[slot, j], recv_sem=recv_sem.at[k],
            device_id={"ep": xor(me, j, n)}, device_id_type=MESH)

    def back_copy(k):
        return pltpu.make_async_remote_copy(
            src_ref=ybuf.at[k], dst_ref=bbuf.at[k], send_sem=ysend_sem.at[k], recv_sem=yrecv_sem.at[k],
            device_id={"ep": xor(me, k, n)}, device_id_type=MESH)

    def put(dst):
        c = pltpu.make_async_copy(temp, dst, lsem.at[1])
        c.start()
        c.wait()

    def gather(positions):
        slot_ids = lax.broadcasted_iota(jnp.int32, (cap, tokens), 0)
        pmat[...] = jnp.where(slot_ids == positions, 1.0, 0.0).astype(bf16)

        def column(c, _):
            cols = pl.ds(pl.multiple_of(c * 512, 512), 512)
            temp[:, cols] = jnp.dot(pmat[...], ubuf[:, cols], preferred_element_type=f32).astype(bf16)
            return 0

        lax.fori_loop(0, ncol, column, 0)

    def dispatch(i, _):
        k = 2 - i + (i // 2) * (5 - i - (i // 3))
        gather(pos_row[pl.ds(k, 1), :])

        @pl.when(k == 0)
        def _():
            put(rbuf.at[0])

        @pl.when(k > 0)
        def _():
            put(sbuf.at[k])
            send_copy(k).start()

        return 0

    lax.fori_loop(0, 4, dispatch, 0)

    def forward(slot):
        far_rows(slot).wait_recv()
        far_slots(slot).wait_recv()
        load = pltpu.make_async_copy(ufar.at[slot], ubuf, lsem.at[0])
        load.start()
        load.wait()

        def target(i, _):
            j = 2 - i + (i // 2) * (5 - i - (i // 3))
            k = xor(6 - 2 * slot, j, n)
            gather(posfar[slot, pl.ds(k, 1), :])

            @pl.when(j == 0)
            def _():
                put(rbuf.at[k])

            @pl.when(j > 0)
            def _():
                put(fbuf.at[slot, j])
                forward_copy(slot, j).start()

            return 0

        lax.fori_loop(0, 4, target, 0)

    def mlp(t, _):
        i, f, slot = t // nf, t % nf, t % 2
        k = visit(i)

        @pl.when((f == 0) & (inner == 0) & (i == 3))
        def _():
            pl.semaphore_wait(go_sem, 2)
            far_rows(1).start()

        @pl.when((f == 0) & (inner == 1) & (i == 3))
        def _():
            far_rows(0).wait_send()
            for j in (2, 3):
                pl.semaphore_signal(go_sem, inc=1, device_id={"ep": xor(me, j, n)}, device_id_type=MESH)

        @pl.when((f == 0) & (inner == 1) & (i % 3 == 0) & (i > 0))
        def _():
            forward(i // 3 - 1)

            @pl.when(i == 6)
            def _():
                back_copy(7).start()

        @pl.when(f == 0)
        def _():
            @pl.when((k > 0) & ((inner == 0) | (k < 4) | (k % 2 == 1)))
            def _():
                back_copy_like = pltpu.make_async_remote_copy(
                    src_ref=ybuf.at[k], dst_ref=rbuf.at[k], send_sem=send_sem.at[0], recv_sem=recv_sem.at[k],
                    device_id={"ep": xor(me, k, n)}, device_id_type=MESH)
                back_copy_like.wait_recv()

            load = pltpu.make_async_copy(rbuf.at[k], xin, lsem.at[1])
            load.start()
            load.wait()
            acc[...] = jnp.zeros_like(acc)

        for c in weight_copies(f, slot):
            c.wait()

        @pl.when(t + 1 < n * nf)
        def _():
            for c in weight_copies((t + 1) % nf, (t + 1) % 2):
                c.start()

        gate_proj = jnp.dot(xin[...], wgb[slot], preferred_element_type=f32)
        up_proj = jnp.dot(xin[...], wub[slot], preferred_element_type=f32)
        inner_act = (jax.nn.silu(gate_proj) * up_proj).astype(bf16)
        for c in range(ncol):
            cols = slice(c * 512, (c + 1) * 512)
            acc[:, cols] += jnp.dot(inner_act, wdb[slot, :, cols], preferred_element_type=f32)

        @pl.when(f == nf - 1)
        def _():
            temp[...] = acc[...].astype(bf16)

            @pl.when(k == 0)
            def _():
                put(bbuf.at[0])

            @pl.when(k > 0)
            def _():
                put(ybuf.at[k])

            @pl.when((k > 0) & ((inner == 0) | (i != 5)))
            def _():
                back_copy(k).start()

        return 0

    lax.fori_loop(0, n * nf, mlp, 0)
    x_copy = pltpu.make_async_copy(x_hbm, ubuf, lsem.at[0])
    x_copy.start()
    x_copy.wait()

    def out_copy(r):
        rows = pl.ds(pl.multiple_of(r * tc, tc), tc)
        return pltpu.make_async_copy(ubuf.at[rows, :], out.at[rows, :], osem.at[r])

    def combine(i, _):
        k = gather_back(i)

        @pl.when(k > 0)
        def _():
            back_copy(k).wait_recv()

        load = pltpu.make_async_copy(bbuf.at[k], xin, lsem.at[1])
        load.start()
        load.wait()

        def rows_step(r, _):
            rows = pl.ds(pl.multiple_of(r * tc, tc), tc)
            lane = lax.broadcasted_iota(jnp.int32, (tc, n), 1)
            pos = jnp.sum(jnp.where(lane == k, pos_col[rows, :], 0), axis=1, keepdims=True)
            gate = jnp.sum(jnp.where(lane == k, gate_col[rows, :], 0.0), axis=1, keepdims=True)
            slot_ids = lax.broadcasted_iota(jnp.int32, (tc, cap), 1)
            pick = jnp.where(slot_ids == pos, 1.0, 0.0).astype(bf16)

            @pl.when(i == 0)
            def _():
                oacc[rows, :] = ubuf[rows, :].astype(f32)

            for c in range(ncol):
                cols = slice(c * 512, (c + 1) * 512)
                picked = jnp.dot(pick, xin[:, cols], preferred_element_type=f32)
                oacc[rows, cols] += gate * picked

            @pl.when(i == n - 1)
            def _():
                ubuf[rows, :] = oacc[rows, :].astype(bf16)
                out_copy(r).start()

            return 0

        lax.fori_loop(0, tokens // tc, rows_step, 0)
        return 0

    lax.fori_loop(0, n, combine, 0)

    def finish(k, _):
        back_copy(k).wait_send()

        @pl.when(k < 4)
        def _():
            send_copy(k).wait_send()

        @pl.when((k < 4) & (inner == 1))
        def _():
            forward_copy(0, k).wait_send()
            forward_copy(1, k).wait_send()

        return 0

    lax.fori_loop(1, n, finish, 0)
    far_slots(0).wait_send()

    @pl.when(inner == 0)
    def _():
        far_rows(0).wait_send()


    def drain(r, _):
        out_copy(r).wait()
        return 0

    lax.fori_loop(0, tokens // tc, drain, 0)


def solution(mesh):
    group_size = mesh.shape["ep"]
    rows_spec = P(("dp", "ep"))

    def device_step(hidden, ln_gamma, ln_beta, w_router, w_gate, w_up, w_down, choice, mask_first, mask_second):
        tokens, width = hidden.shape
        n = group_size
        ff = w_gate.shape[2]
        cap = (10 * tokens + 4 * n - 1) // (4 * n)
        ft, tc = 512, 256
        normed = layer_norm(hidden, ln_gamma, ln_beta)
        gate_vals = sparse_gates(normed, w_router, choice, mask_first, mask_second)
        experts = lax.axis_index("ep").astype(jnp.int32) ^ jnp.arange(n, dtype=jnp.int32)
        hit = choice[..., None] == experts
        hit_any = jnp.sum(hit.astype(jnp.int32), axis=1)
        before = jnp.cumsum(hit_any, axis=0) - hit_any
        kept = (hit_any > 0) & (before < cap)
        pos = jnp.where(kept, before, -1)
        gates = jnp.where(kept, jnp.sum(jnp.where(hit, gate_vals[..., None], 0.0), axis=1), 0.0)
        block = jax.ShapeDtypeStruct((n, cap, width), jnp.bfloat16)
        near = jax.ShapeDtypeStruct((n // 2, cap, width), jnp.bfloat16)
        far_rows = jax.ShapeDtypeStruct((2, tokens, width), jnp.bfloat16)
        far_blocks = jax.ShapeDtypeStruct((2, n // 2, cap, width), jnp.bfloat16)
        vmem = pl.BlockSpec(memory_space=pltpu.VMEM)
        hbm = pl.BlockSpec(memory_space=pl.ANY)
        bf16, f32 = jnp.bfloat16, jnp.float32
        return pl.pallas_call(
            functools.partial(moe_kernel, n, cap, ft, tc),
            out_shape=(jax.ShapeDtypeStruct((tokens, width), bf16), near, block, block, block, far_rows, far_blocks),
            in_specs=[vmem] * 3 + [hbm] * 5,
            out_specs=(hbm,) * 7,
            scratch_shapes=[
                pltpu.VMEM((tokens, width), bf16),
                pltpu.VMEM((cap, tokens), bf16),
                pltpu.VMEM((cap, width), bf16),
                pltpu.VMEM((cap, width), bf16),
                pltpu.VMEM((cap, width), f32),
                pltpu.VMEM((2, width, ft), bf16),
                pltpu.VMEM((2, width, ft), bf16),
                pltpu.VMEM((2, ft, width), bf16),
                pltpu.VMEM((tokens, width), f32),
                pltpu.VMEM((2, n, tokens), jnp.int32),
                pltpu.SemaphoreType.DMA((n,)),
                pltpu.SemaphoreType.DMA((n,)),
                pltpu.SemaphoreType.DMA((n,)),
                pltpu.SemaphoreType.DMA((n,)),
                pltpu.SemaphoreType.DMA((2,)),
                pltpu.SemaphoreType.DMA((2, 2)),
                pltpu.SemaphoreType.DMA((2, n // 2)),
                pltpu.SemaphoreType.DMA((2, 3)),
                pltpu.SemaphoreType.DMA((2,)),
                pltpu.SemaphoreType.DMA((tokens // tc,)),
                pltpu.SemaphoreType.REGULAR,
            ],
            compiler_params=pltpu.CompilerParams(
                collective_id=0, has_side_effects=True, vmem_limit_bytes=67043328),
            cost_estimate=pl.CostEstimate(
                flops=6 * n * cap * width * ff, bytes_accessed=n * 6 * width * ff, transcendentals=0),
        )(pos.T, pos, gates, normed, hidden, w_gate[0], w_up[0], w_down[0])[0]

    return jax.shard_map(device_step, mesh=mesh,
                         in_specs=(rows_spec, P(), P(), P(), P("ep"), P("ep"), P("ep"), rows_spec, rows_spec, rows_spec),
                         out_specs=rows_spec, check_vma=False)
```

```python
import functools

import jax
import jax.numpy as jnp
from jax import lax
from jax.experimental import pallas as pl
from jax.experimental.pallas import tpu as pltpu
from jax.sharding import PartitionSpec as P

LN_EPS = 1e-5
MESH = pl.DeviceIdType.MESH


def norm_kernel(x_ref, gamma_ref, beta_ref, out_ref):
    values = x_ref[...].astype(jnp.float32)
    centred = values - jnp.mean(values, axis=-1, keepdims=True)
    variance = jnp.mean(centred * centred, axis=-1, keepdims=True)
    out_ref[...] = (centred * lax.rsqrt(variance + LN_EPS) * gamma_ref[...] + beta_ref[...]).astype(jnp.bfloat16)


def layer_norm(token_rows, ln_gamma, ln_beta):
    tokens, width = token_rows.shape
    rows = pl.BlockSpec((256, width), lambda i: (i, 0))
    whole = pl.BlockSpec((1, width), lambda i: (0, 0))
    return pl.pallas_call(
        norm_kernel,
        grid=(tokens // 256,),
        out_shape=jax.ShapeDtypeStruct((tokens, width), jnp.bfloat16),
        in_specs=[rows, whole, whole],
        out_specs=rows,
        compiler_params=pltpu.CompilerParams(vmem_limit_bytes=32 << 20),
        cost_estimate=pl.CostEstimate(flops=8 * tokens * width, bytes_accessed=4 * tokens * width, transcendentals=tokens),
    )(token_rows, ln_gamma[None, :], ln_beta[None, :])


def sparse_gates(normed, w_router, choice, mask_first, mask_second):
    scores = jnp.dot(normed, w_router, preferred_element_type=jnp.float32)
    expert_ids = jnp.arange(w_router.shape[1], dtype=jnp.int32)
    mask_pair = jnp.stack([mask_first, mask_second], axis=1) > 0
    soft_probs = jax.nn.softmax(jnp.where(mask_pair, scores[:, None, :], -jnp.inf), axis=-1)
    return jnp.sum(jnp.where(choice[:, :, None] == expert_ids, soft_probs, 0.0), axis=-1)


def xor(a, b, n):
    total, bit = 0, 1
    while bit < n:
        p, q = (a // bit) % 2, (b // bit) % 2
        total = total + bit * (p + q - 2 * p * q)
        bit *= 2
    return total


def moe_kernel(n, cap, ft, tc, pos_row, pos_col, gate_col, u_hbm, x_hbm, wg, wu, wd,
               out, sbuf, rbuf, ybuf, bbuf, ufar, fbuf,
               ubuf, pmat, temp, xin, acc, wgb, wub, wdb, oacc, posfar,
               send_sem, recv_sem, ysend_sem, yrecv_sem, usend_sem, urecv_sem, fsend_sem, wsem, lsem, osem, go_sem):
    me = lax.axis_index("ep")
    tokens, width = ubuf.shape
    nf = wg.shape[1] // ft
    ncol = width // 512
    bf16, f32 = jnp.bfloat16, jnp.float32
    inner = ((me // 2 + 1) // 2) % 2

    def visit(i):
        return i + inner * (i // 4) * (2 - 4 * ((i // 2) % 2))

    def gather_back(i):
        return i + (1 - inner) * (i // 4) * (2 - 4 * ((i // 2) % 2))

    u_copy = pltpu.make_async_copy(u_hbm, ubuf, lsem.at[0])
    u_copy.start()

    def weight_copies(f, slot):
        cols = pl.ds(pl.multiple_of(f * ft, ft), ft)
        return (pltpu.make_async_copy(wg.at[:, cols], wgb.at[slot], wsem.at[slot, 0]),
                pltpu.make_async_copy(wu.at[:, cols], wub.at[slot], wsem.at[slot, 1]),
                pltpu.make_async_copy(wd.at[cols, :], wdb.at[slot], wsem.at[slot, 2]))

    for c in weight_copies(0, 0):
        c.start()

    barrier = pltpu.get_barrier_semaphore()

    def greet(k, _):
        pl.semaphore_signal(barrier, inc=1, device_id={"ep": xor(me, k, n)}, device_id_type=MESH)
        return 0

    lax.fori_loop(1, n, greet, 0)
    pl.semaphore_wait(barrier, n - 1)

    def far_rows(slot):
        return pltpu.make_async_remote_copy(
            src_ref=u_hbm, dst_ref=ufar.at[slot], send_sem=usend_sem.at[0], recv_sem=urecv_sem.at[slot, 0],
            device_id={"ep": xor(me, 4 + 2 * inner, n)}, device_id_type=MESH)

    def far_slots(slot):
        return pltpu.make_async_remote_copy(
            src_ref=pos_row, dst_ref=posfar.at[slot], send_sem=usend_sem.at[1], recv_sem=urecv_sem.at[slot, 1],
            device_id={"ep": xor(me, 4 + 2 * inner, n)}, device_id_type=MESH)

    @pl.when(inner == 1)
    def _():
        far_rows(0).start()

    far_slots(1 - inner).start()
    u_copy.wait()

    def send_copy(k):
        return pltpu.make_async_remote_copy(
            src_ref=sbuf.at[k], dst_ref=rbuf.at[k], send_sem=send_sem.at[k], recv_sem=recv_sem.at[k],
            device_id={"ep": xor(me, k, n)}, device_id_type=MESH)

    def forward_copy(slot, j):
        k = xor(6 - 2 * slot, j, n)
        return pltpu.make_async_remote_copy(
            src_ref=fbuf.at[slot, j], dst_ref=rbuf.at[k], send_sem=fsend_sem.at[slot, j], recv_sem=recv_sem.at[k],
            device_id={"ep": xor(me, j, n)}, device_id_type=MESH)

    def back_copy(k):
        return pltpu.make_async_remote_copy(
            src_ref=ybuf.at[k], dst_ref=bbuf.at[k], send_sem=ysend_sem.at[k], recv_sem=yrecv_sem.at[k],
            device_id={"ep": xor(me, k, n)}, device_id_type=MESH)

    def put(dst):
        c = pltpu.make_async_copy(temp, dst, lsem.at[1])
        c.start()
        c.wait()

    def gather(positions):
        slot_ids = lax.broadcasted_iota(jnp.int32, (cap, tokens), 0)
        pmat[...] = jnp.where(slot_ids == positions, 1.0, 0.0).astype(bf16)

        def column(c, _):
            cols = pl.ds(pl.multiple_of(c * 512, 512), 512)
            temp[:, cols] = jnp.dot(pmat[...], ubuf[:, cols], preferred_element_type=f32).astype(bf16)
            return 0

        lax.fori_loop(0, ncol, column, 0)

    def dispatch(i, _):
        k = 2 - i + (i // 2) * (5 - i - (i // 3))
        gather(pos_row[pl.ds(k, 1), :])

        @pl.when(k == 0)
        def _():
            put(rbuf.at[0])

        @pl.when(k > 0)
        def _():
            put(sbuf.at[k])
            send_copy(k).start()

        return 0

    lax.fori_loop(0, 4, dispatch, 0)

    def forward(slot):
        far_rows(slot).wait_recv()
        far_slots(slot).wait_recv()
        load = pltpu.make_async_copy(ufar.at[slot], ubuf, lsem.at[0])
        load.start()
        load.wait()

        def target(i, _):
            j = 2 - i + (i // 2) * (5 - i - (i // 3))
            k = xor(6 - 2 * slot, j, n)
            gather(posfar[slot, pl.ds(k, 1), :])

            @pl.when(j == 0)
            def _():
                put(rbuf.at[k])

            @pl.when(j > 0)
            def _():
                put(fbuf.at[slot, j])
                forward_copy(slot, j).start()

            return 0

        lax.fori_loop(0, 4, target, 0)

    def mlp(t, _):
        i, f, slot = t // nf, t % nf, t % 2
        k = visit(i)

        @pl.when((f == 0) & (inner == 0) & (i == 3))
        def _():
            pl.semaphore_wait(go_sem, 2)
            far_rows(1).start()

        @pl.when((f == 0) & (inner == 1) & (i == 3))
        def _():
            far_rows(0).wait_send()
            for j in (2, 3):
                pl.semaphore_signal(go_sem, inc=1, device_id={"ep": xor(me, j, n)}, device_id_type=MESH)

        @pl.when((f == 0) & (inner == 1) & (i % 3 == 0) & (i > 0))
        def _():
            forward(i // 3 - 1)

            @pl.when(i == 6)
            def _():
                back_copy(7).start()

        @pl.when(f == 0)
        def _():
            @pl.when((k > 0) & ((inner == 0) | (k < 4) | (k % 2 == 1)))
            def _():
                back_copy_like = pltpu.make_async_remote_copy(
                    src_ref=ybuf.at[k], dst_ref=rbuf.at[k], send_sem=send_sem.at[0], recv_sem=recv_sem.at[k],
                    device_id={"ep": xor(me, k, n)}, device_id_type=MESH)
                back_copy_like.wait_recv()

            load = pltpu.make_async_copy(rbuf.at[k], xin, lsem.at[1])
            load.start()
            load.wait()
            acc[...] = jnp.zeros_like(acc)

        for c in weight_copies(f, slot):
            c.wait()

        @pl.when(t + 1 < n * nf)
        def _():
            for c in weight_copies((t + 1) % nf, (t + 1) % 2):
                c.start()

        gate_proj = jnp.dot(xin[...], wgb[slot], preferred_element_type=f32)
        up_proj = jnp.dot(xin[...], wub[slot], preferred_element_type=f32)
        inner_act = (jax.nn.silu(gate_proj) * up_proj).astype(bf16)
        for c in range(ncol):
            cols = slice(c * 512, (c + 1) * 512)
            acc[:, cols] += jnp.dot(inner_act, wdb[slot, :, cols], preferred_element_type=f32)

        @pl.when(f == nf - 1)
        def _():
            temp[...] = acc[...].astype(bf16)

            @pl.when(k == 0)
            def _():
                put(bbuf.at[0])

            @pl.when(k > 0)
            def _():
                put(ybuf.at[k])

            @pl.when((k > 0) & ((inner == 0) | (i != 5)))
            def _():
                back_copy(k).start()

        return 0

    lax.fori_loop(0, n * nf, mlp, 0)
    x_copy = pltpu.make_async_copy(x_hbm, ubuf, lsem.at[0])
    x_copy.start()
    x_copy.wait()

    def out_copy(r):
        rows = pl.ds(pl.multiple_of(r * tc, tc), tc)
        return pltpu.make_async_copy(ubuf.at[rows, :], out.at[rows, :], osem.at[r])

    def combine(i, _):
        k = gather_back(i)

        @pl.when(k > 0)
        def _():
            back_copy(k).wait_recv()

        load = pltpu.make_async_copy(bbuf.at[k], xin, lsem.at[1])
        load.start()
        load.wait()

        def rows_step(r, _):
            rows = pl.ds(pl.multiple_of(r * tc, tc), tc)
            lane = lax.broadcasted_iota(jnp.int32, (tc, n), 1)
            pos = jnp.sum(jnp.where(lane == k, pos_col[rows, :], 0), axis=1, keepdims=True)
            gate = jnp.sum(jnp.where(lane == k, gate_col[rows, :], 0.0), axis=1, keepdims=True)
            slot_ids = lax.broadcasted_iota(jnp.int32, (tc, cap), 1)
            pick = jnp.where(slot_ids == pos, 1.0, 0.0).astype(bf16)

            @pl.when(i == 0)
            def _():
                oacc[rows, :] = ubuf[rows, :].astype(f32)

            for c in range(ncol):
                cols = slice(c * 512, (c + 1) * 512)
                picked = jnp.dot(pick, xin[:, cols], preferred_element_type=f32)
                oacc[rows, cols] += gate * picked

            @pl.when(i == n - 1)
            def _():
                ubuf[rows, :] = oacc[rows, :].astype(bf16)
                out_copy(r).start()

            return 0

        lax.fori_loop(0, tokens // tc, rows_step, 0)
        return 0

    lax.fori_loop(0, n, combine, 0)

    def finish(k, _):
        back_copy(k).wait_send()

        @pl.when(k < 4)
        def _():
            send_copy(k).wait_send()

        @pl.when((k < 4) & (inner == 1))
        def _():
            forward_copy(0, k).wait_send()
            forward_copy(1, k).wait_send()

        return 0

    lax.fori_loop(1, n, finish, 0)
    far_slots(0).wait_send()

    @pl.when(inner == 0)
    def _():
        far_rows(0).wait_send()


    def drain(r, _):
        out_copy(r).wait()
        return 0

    lax.fori_loop(0, tokens // tc, drain, 0)


def solution(mesh):
    group_size = mesh.shape["ep"]
    rows_spec = P(("dp", "ep"))

    def device_step(hidden, ln_gamma, ln_beta, w_router, w_gate, w_up, w_down, choice, mask_first, mask_second):
        tokens, width = hidden.shape
        n = group_size
        ff = w_gate.shape[2]
        cap = (10 * tokens + 4 * n - 1) // (4 * n)
        ft, tc = 512, 256
        normed = layer_norm(hidden, ln_gamma, ln_beta)
        gate_vals = sparse_gates(normed, w_router, choice, mask_first, mask_second)
        experts = lax.axis_index("ep").astype(jnp.int32) ^ jnp.arange(n, dtype=jnp.int32)
        hit = choice[..., None] == experts
        hit_any = jnp.sum(hit.astype(jnp.int32), axis=1)
        before = jnp.cumsum(hit_any, axis=0) - hit_any
        kept = (hit_any > 0) & (before < cap)
        pos = jnp.where(kept, before, -1)
        gates = jnp.where(kept, jnp.sum(jnp.where(hit, gate_vals[..., None], 0.0), axis=1), 0.0)
        block = jax.ShapeDtypeStruct((n, cap, width), jnp.bfloat16)
        near = jax.ShapeDtypeStruct((n // 2, cap, width), jnp.bfloat16)
        far_rows = jax.ShapeDtypeStruct((2, tokens, width), jnp.bfloat16)
        far_blocks = jax.ShapeDtypeStruct((2, n // 2, cap, width), jnp.bfloat16)
        vmem = pl.BlockSpec(memory_space=pltpu.VMEM)
        hbm = pl.BlockSpec(memory_space=pl.ANY)
        bf16, f32 = jnp.bfloat16, jnp.float32
        return pl.pallas_call(
            functools.partial(moe_kernel, n, cap, ft, tc),
            out_shape=(jax.ShapeDtypeStruct((tokens, width), bf16), near, block, block, block, far_rows, far_blocks),
            in_specs=[vmem] * 3 + [hbm] * 5,
            out_specs=(hbm,) * 7,
            scratch_shapes=[
                pltpu.VMEM((tokens, width), bf16),
                pltpu.VMEM((cap, tokens), bf16),
                pltpu.VMEM((cap, width), bf16),
                pltpu.VMEM((cap, width), bf16),
                pltpu.VMEM((cap, width), f32),
                pltpu.VMEM((2, width, ft), bf16),
                pltpu.VMEM((2, width, ft), bf16),
                pltpu.VMEM((2, ft, width), bf16),
                pltpu.VMEM((tokens, width), f32),
                pltpu.VMEM((2, n, tokens), jnp.int32),
                pltpu.SemaphoreType.DMA((n,)),
                pltpu.SemaphoreType.DMA((n,)),
                pltpu.SemaphoreType.DMA((n,)),
                pltpu.SemaphoreType.DMA((n,)),
                pltpu.SemaphoreType.DMA((2,)),
                pltpu.SemaphoreType.DMA((2, 2)),
                pltpu.SemaphoreType.DMA((2, n // 2)),
                pltpu.SemaphoreType.DMA((2, 3)),
                pltpu.SemaphoreType.DMA((2,)),
                pltpu.SemaphoreType.DMA((tokens // tc,)),
                pltpu.SemaphoreType.REGULAR,
            ],
            compiler_params=pltpu.CompilerParams(
                collective_id=0, has_side_effects=True, vmem_limit_bytes=67043328),
            cost_estimate=pl.CostEstimate(
                flops=6 * n * cap * width * ff, bytes_accessed=n * 6 * width * ff, transcendentals=0),
        )(pos.T, pos, gates, normed, hidden, w_gate[0], w_up[0], w_down[0])[0]

    return jax.shard_map(device_step, mesh=mesh,
                         in_specs=(rows_spec, P(), P(), P(), P("ep"), P("ep"), P("ep"), rows_spec, rows_spec, rows_spec),
                         out_specs=rows_spec, check_vma=False)
```
